256 devices in a mesh: tm: 64 (over z, y, core), freq: 4 (over x).
Axes of the slice: x: 4, y: 4, z: 8, core: 2. Of those that a mesh axis runs over, the one named last changes fastest.
Arguments:
- snapshots: bfloat16 [4352, 3, 32768], P('tm', None, 'freq'), may hold values from -200 to 200
- block_starts: int32 [32], replicated, may hold values from 0 to 4032, as said below
- freq_index: int32 [16], replicated, may hold values from 0 to 128
Outputs:
- modes: bfloat16 [16, 32, 2, 3, 32768], P(None, None, None, None, ('freq', 'tm'))
- energy: float32 [16], replicated
The draws below stay inside these ranges and needn't reach their ends.
Inputs may be any that keep to these rules, and one draw needn't show every extreme that they name: `block_starts`: block b starts at b * 128 plus between 0 and 64.
All inputs are finite; a program needn't handle non-finite values.
Results may differ from the reference program's by a relative error of at most 0.0085.
Values may be sent and summed in bfloat16 or wider, within the bound.
No kernel may reach another device: no remote copies, remote signals or barrier semaphores. Data moves between devices by JAX's collectives and lax.ppermute only.
A program may use at most 64 MiB of HBM per device.

```python
import math
import jax
import jax.numpy as jnp
from jax import lax

NB = 32
NFFT = 256
NF = 16
HOP = 128
JIT = 64
TT = 4352
NSIT = 6
P_DEV = 128
P_SIZE = 32768


def draw_snapshots(key, part):
    key_noise, key_space, key_time = jax.random.split(key, 3)
    rising = jnp.exp(math.log(3.0) * jnp.arange(P_SIZE, dtype=jnp.float32) / P_SIZE)
    space_scale = rising * jnp.exp(jax.random.uniform(key_space, (P_SIZE,), minval=0.0, maxval=math.log(10.0))) / 3.0
    time_scale = jnp.exp(jax.random.uniform(key_time, (TT,), minval=math.log(0.3), maxval=math.log(3.0)))
    values = jnp.clip(jax.random.normal(key_noise, (TT, 3, P_SIZE)), -5.0, 5.0)
    return (values * time_scale[:, None, None] * space_scale[None, None, :]).astype(jnp.bfloat16)


def draw_block_starts(key, part):
    jitter = jax.random.randint(key, (NB,), 0, JIT + 1)
    return (jnp.arange(NB, dtype=jnp.int32) * HOP + jitter).astype(jnp.int32)


def set_ends(drawn, rng, low, top_value):
    dims = drawn.shape
    index_at = [jax.random.randint(jax.random.fold_in(rng, axis), (), 0, dims[axis]) for axis in range(len(dims))]
    drawn = drawn.at[tuple(index_at)].set(low)
    longest = dims.index(max(dims))
    index_at[longest] = (index_at[longest] + 1) % dims[longest]
    return drawn.at[tuple(index_at)].set(top_value)


def setup_inputs(seed: int = 0) -> dict:
    key_list = jax.random.split(jax.random.key(seed), 4)
    return {
        "snapshots": draw_snapshots(jax.random.fold_in(key_list[3], 71), 0),
        "block_starts": draw_block_starts(jax.random.fold_in(key_list[3], 71), 0),
        "freq_index": set_ends(jax.random.randint(key_list[2], (NF,), 0, NFFT // 2 + 1), jax.random.fold_in(key_list[2], 1), 0, (NFFT // 2 + 1) - 1).astype(jnp.int32),
    }


def dft_rows(freq_index):
    times_idx = jnp.arange(NFFT, dtype=jnp.int32)
    phase_int = freq_index[:, None].astype(jnp.int32) * times_idx[None, :] % NFFT
    angles = 2.0 * math.pi / NFFT * phase_int.astype(jnp.float32)
    window = 0.5 - 0.5 * jnp.cos(2.0 * math.pi / NFFT * times_idx.astype(jnp.float32))
    scaling = 1.0 / jnp.sqrt(jnp.sum(window * window))
    cosine = window[None, :] * jnp.cos(angles) * scaling
    sine_rows = -window[None, :] * jnp.sin(angles) * scaling
    return jnp.stack([cosine, sine_rows], 1).reshape(2 * NF, NFFT).astype(jnp.bfloat16)

def block_rows(block_starts):
    return block_starts[:, None].astype(jnp.int32) + jnp.arange(NFFT, dtype=jnp.int32)[None, :]

def matmul_batch(left, right):
    return jnp.einsum('fij,fjk->fik', left, right, precision=lax.Precision.HIGHEST)

def whiten(summed, points):
    gram_re = summed[:, 0]
    gram_im = summed[:, 1]
    top_rows = jnp.concatenate([gram_re, -gram_im], 2)
    low_rows = jnp.concatenate([gram_im, gram_re], 2)
    hermit = jnp.concatenate([top_rows, low_rows], 1)
    frob = jnp.sqrt(lax.optimization_barrier(jnp.sum(hermit * hermit, axis=(1, 2))) + 1e-06)
    identity = jnp.eye(2 * NB, dtype=jnp.float32)[None]
    iterate = hermit / frob[:, None, None]
    inverse = jnp.broadcast_to(identity, hermit.shape)
    for iteration in range(NSIT):
        factor = 1.5 * identity - 0.5 * matmul_batch(inverse, iterate)
        iterate = matmul_batch(iterate, factor)
        inverse = matmul_batch(factor, inverse)
    columns = inverse[:, :, :NB] * jnp.sqrt(6.0 * points / frob)[:, None, None]
    upper = columns[:, :NB]
    lower = columns[:, NB:]
    coefficients = jnp.stack([jnp.stack([upper, -lower], 1), jnp.stack([lower, upper], 1)], 1)
    energy = jnp.trace(gram_re, axis1=1, axis2=2) / (3.0 * NB * points)
    return (coefficients, energy)

def reference(snapshots, block_starts, freq_index):
    dft_table = dft_rows(freq_index).astype(jnp.float32)
    offsets = block_rows(block_starts)
    columns_all = snapshots.reshape(TT, 3 * P_SIZE)
    block_cols = 16 * P_DEV

    def spectra_block(start):
        piece = lax.dynamic_slice_in_dim(columns_all, start, block_cols, 1)
        windows = jnp.take(piece, offsets, axis=0).astype(jnp.float32)
        return jnp.einsum('rt,btn->brn', dft_table, windows, precision=lax.Precision.HIGHEST).astype(jnp.bfloat16)
    starts = jnp.arange(3 * P_SIZE // block_cols, dtype=jnp.int32) * block_cols
    pieces = lax.map(spectra_block, starts)
    spectra = jnp.transpose(pieces, (1, 2, 0, 3)).reshape(NB, NF, 2, 3 * P_SIZE)
    by_freq = jnp.moveaxis(spectra, 1, 0)

    def gram_one(spec_f):
        real_part = spec_f[:, 0].astype(jnp.float32)
        imag_part = spec_f[:, 1].astype(jnp.float32)
        gram_re = jnp.dot(real_part, real_part.T, precision=lax.Precision.HIGHEST) + jnp.dot(imag_part, imag_part.T, precision=lax.Precision.HIGHEST)
        cross_terms = jnp.dot(real_part, imag_part.T, precision=lax.Precision.HIGHEST)
        return jnp.stack([gram_re, cross_terms - cross_terms.T])
    summed = lax.map(gram_one, by_freq)
    coefficients, energy = whiten(summed, float(P_SIZE))
    coef_bf = coefficients.astype(jnp.bfloat16)

    def modes_one(pair):
        coef_f, spec_f = pair
        return jnp.einsum('orbj,brn->jon', coef_f.astype(jnp.float32), spec_f.astype(jnp.float32), precision=lax.Precision.HIGHEST).astype(jnp.bfloat16)
    modes = lax.map(modes_one, (coef_bf, by_freq))
    return (modes.reshape(NF, NB, 2, 3, P_SIZE), energy)
```

```python
import functools
import math

import jax
import jax.numpy as jnp
from jax import lax
from jax.experimental import pallas as pl
from jax.experimental.pallas import tpu as pltpu
from jax.sharding import Mesh
from jax.sharding import PartitionSpec as P


NB = 32
NFFT = 256
NF = 16
HOP = 128
JIT = 64
NSIT = 6
NC = 3
LANES = 128

NZ, NY, NCORE, NX = 8, 4, 2, 4
NYC = NY * NCORE
T_DEV = 68
T_PAD = 72
T_SLAB = T_DEV * NYC
KDIM = NYC * T_PAD
BASE = [max(0, (T_SLAB * z - NFFT - JIT) // HOP + 1) for z in range(NZ)]
TOP = [min(NB, -(-(T_SLAB * (z + 1)) // HOP)) for z in range(NZ)]
BLK = max(t - b for b, t in zip(BASE, TOP))
NG = 4
FG = NF // NG
GROWS = BLK * FG * 2
ROWS = NG * GROWS
SROWS = FG * 2 * NB
CHUNKS = ((0, 1), (2,))

YSTEPS = ((0, 0), (1, 0), (3, 0), (2, 0), (1, 1), (3, 1), (2, 1), (0, 1))
ZSTEPS = (0, 1, 7, 2, 6, 3, 5, 4)

VMEM = pl.BlockSpec(memory_space=pltpu.VMEM)
SMEM = pl.BlockSpec(memory_space=pltpu.SMEM)
F32 = jnp.float32
BF16 = jnp.bfloat16


def params():
    return pltpu.CompilerParams(vmem_limit_bytes=48 * 1024 * 1024)


def cost(flops, nbytes):
    return pl.CostEstimate(flops=int(flops), bytes_accessed=int(nbytes), transcendentals=0)


def pack_kernel(x_ref, *outs):
    _, dests, _, _, _ = place()
    for k in range(NYC):
        for zz in range(NZ):
            lane = pl.multiple_of((dests[k] + NYC * zz) * LANES, LANES)
            outs[k][0, :T_DEV, zz * LANES : (zz + 1) * LANES] = x_ref[0, :, pl.ds(lane, LANES)]
        outs[k][0, T_DEV:, :] = jnp.zeros((T_PAD - T_DEV, NZ * LANES), BF16)


def pack(x, comps):
    nc = len(comps)
    first = comps[0]
    return pl.pallas_call(
        pack_kernel,
        grid=(nc,),
        in_specs=[pl.BlockSpec((1, T_DEV, x.shape[2]), lambda i: (first + i, 0, 0))],
        out_specs=[pl.BlockSpec((1, T_PAD, NZ * LANES), lambda i: (i, 0, 0))] * NYC,
        out_shape=[jax.ShapeDtypeStruct((nc, T_PAD, NZ * LANES), BF16)] * NYC,
        compiler_params=params(),
        cost_estimate=cost(2e6 * nc, 2.3e6 * nc),
        name="pack",
    )(x)


def send_yc(array, k):
    dy, dc = YSTEPS[k]
    if k == 0:
        return array
    pairs = [
        (y * NCORE + c, ((y + dy) % NY) * NCORE + (c ^ dc)) for y in range(NY) for c in range(NCORE)
    ]
    return lax.ppermute(array, ("y", "c"), pairs)


def send_z(array, k):
    dz = ZSTEPS[k]
    if k == 0:
        return array
    return lax.ppermute(array, "z", [(i, (i + dz) % NZ) for i in range(NZ)])


def dft_rows(freq_index):
    times_idx = jnp.arange(NFFT, dtype=jnp.int32)
    phase_int = freq_index[:, None] * times_idx[None, :] % NFFT
    angles = 2.0 * math.pi / NFFT * phase_int.astype(F32)
    window = 0.5 - 0.5 * jnp.cos(2.0 * math.pi / NFFT * times_idx.astype(F32))
    scaling = 1.0 / jnp.sqrt(jnp.sum(window * window))
    cosine = window[None, :] * jnp.cos(angles) * scaling
    sine_rows = -window[None, :] * jnp.sin(angles) * scaling
    return jnp.stack([cosine, sine_rows], 1).reshape(2 * NF, NFFT).astype(BF16)


def place():
    zi, yi, ci = (lax.axis_index(a).astype(jnp.int32) for a in ("z", "y", "c"))
    ydests = [lax.rem(yi + dy, NY) * NCORE + (ci ^ dc) for dy, dc in YSTEPS]
    ysrcs = [lax.rem(yi + NY - dy, NY) * NCORE + (ci ^ dc) for dy, dc in YSTEPS]
    zdests = [lax.rem(zi + dz, NZ) for dz in ZSTEPS]
    zsrcs = [lax.rem(zi + NZ - dz, NZ) for dz in ZSTEPS]
    return zi, ydests, ysrcs, zdests, zsrcs


def base_of(z):
    base = jnp.int32(BASE[0])
    for i in range(1, NZ):
        base = jnp.where(z == i, BASE[i], base)
    return base


def tables_kernel(start_ref, table_ref, w_ref, place_ref):
    zi, _, ysrcs, _, zsrcs = place()
    col = lax.broadcasted_iota(jnp.int32, (1, KDIM), 1)
    when = jnp.zeros((1, KDIM), jnp.int32)
    for k in range(NYC):
        step = col - k * T_PAD
        now = jnp.where(step < T_DEV, T_SLAB * zi + T_DEV * ysrcs[k] + step, -(1 << 20))
        when = jnp.where((step >= 0) & (step < T_PAD), now, when)
    tau = lax.broadcasted_iota(jnp.int32, (NFFT, KDIM), 0)
    base = base_of(zi)
    for blk in range(BLK):
        block = base + blk
        start = jnp.where(block < NB, start_ref[jnp.minimum(block, NB - 1)], 1 << 20)
        chosen = jnp.where(tau == when - start, 1.0, 0.0).astype(BF16)
        rows = jnp.dot(table_ref[...], chosen, preferred_element_type=F32).astype(BF16)
        for g in range(NG):
            w_ref[g * GROWS + blk * 2 * FG : g * GROWS + (blk + 1) * 2 * FG, :] = rows[
                g * 2 * FG : (g + 1) * 2 * FG
            ]
    row = lax.broadcasted_iota(jnp.int32, (SROWS, NZ * GROWS), 0)
    wide = lax.broadcasted_iota(jnp.int32, (1, NZ * GROWS), 1)
    meets = jnp.full((1, NZ * GROWS), -1, jnp.int32)
    for k in range(NZ):
        rest = wide - k * GROWS
        block = base_of(zsrcs[k]) + (rest >> 3)
        mine = jnp.where(block < NB, block + ((rest & 7) << 5), -1)
        meets = jnp.where((rest >= 0) & (rest < GROWS), mine, meets)
    place_ref[...] = jnp.where(row == meets, 1.0, 0.0).astype(BF16)


def tables(block_starts, table):
    return pl.pallas_call(
        tables_kernel,
        in_specs=[SMEM, VMEM],
        out_specs=[VMEM, VMEM],
        out_shape=[
            jax.ShapeDtypeStruct((ROWS, KDIM), BF16),
            jax.ShapeDtypeStruct((SROWS, NZ * GROWS), BF16),
        ],
        compiler_params=params(),
        cost_estimate=cost(4e7, 1e6),
        name="tables",
    )(block_starts, table)


def dft_kernel(nc, w_ref, *refs):
    _, _, _, dests, _ = place()
    ins, outs = refs[:NYC], refs[NYC : NYC + NZ]
    data, spec = refs[NYC + NZ :]
    for i in range(nc):
        for k in range(NYC):
            data[k * T_PAD : (k + 1) * T_PAD, :] = ins[k][i]
        for n in range(NZ // 2):
            part = jnp.dot(
                w_ref[...],
                data[:, n * 2 * LANES : (n + 1) * 2 * LANES],
                preferred_element_type=F32,
            ).astype(BF16)
            spec[2 * n] = part[:, :LANES]
            spec[2 * n + 1] = part[:, LANES:]
        for k in range(NZ):
            outs[k][i] = spec[dests[k]]


def dft(w, parts):
    nc = parts[0].shape[0]
    return pl.pallas_call(
        functools.partial(dft_kernel, nc),
        in_specs=[VMEM] * (1 + NYC),
        out_specs=[VMEM] * NZ,
        out_shape=[jax.ShapeDtypeStruct((nc, ROWS, LANES), BF16)] * NZ,
        scratch_shapes=[
            pltpu.VMEM((KDIM, NZ * LANES), BF16),
            pltpu.VMEM((NZ, ROWS, LANES), BF16),
        ],
        compiler_params=params(),
        cost_estimate=cost(2 * ROWS * KDIM * NZ * LANES * nc, 2e6 * nc),
        name="dft",
    )(w, *parts)


def gram_kernel(place_ref, *refs):
    nin = NZ * len(CHUNKS)
    ins, (spec_ref, gram_ref), (parts,) = refs[:nin], refs[nin : nin + 2], refs[nin + 2 :]
    rows = lax.broadcasted_iota(jnp.int32, (NB, NB), 0)
    cols = lax.broadcasted_iota(jnp.int32, (NB, NB), 1)
    for g in range(NG):
        for k in range(NZ):
            for q, comps in enumerate(CHUNKS):
                for i, c in enumerate(comps):
                    parts[k * GROWS : (k + 1) * GROWS, c * LANES : (c + 1) * LANES] = ins[
                        q * NZ + k
                    ][i, g * GROWS : (g + 1) * GROWS, :]
        spec = jnp.dot(place_ref[...], parts[...], preferred_element_type=F32).astype(BF16)
        for f in range(FG):
            for c in range(NC):
                spec_ref[g * FG + f, c * 2 * NB : (c + 1) * 2 * NB, :] = spec[
                    f * 2 * NB : (f + 1) * 2 * NB, c * LANES : (c + 1) * LANES
                ]
        packed = []
        for f in range(FG):
            one = spec[f * 2 * NB : (f + 1) * 2 * NB]
            full = lax.dot_general(one, one, (((1,), (1,)), ((), ())), preferred_element_type=F32)
            real = full[:NB, :NB] + full[NB:, NB:]
            imag = full[:NB, NB:] - full[NB:, :NB]
            packed.append(jnp.where(rows >= cols, real, imag))
        for h in range(FG // 2):
            a, b = packed[2 * h], packed[2 * h + 1]
            gram_ref[g * FG // 2 + h] = jnp.concatenate(
                [a[: NB // 2], a[NB // 2 :], b[: NB // 2], b[NB // 2 :]], axis=1
            )


def gram(placed, parts):
    return pl.pallas_call(
        gram_kernel,
        in_specs=[VMEM] * (1 + len(parts)),
        out_specs=[VMEM, VMEM],
        out_shape=[
            jax.ShapeDtypeStruct((NF, NC * 2 * NB, LANES), BF16),
            jax.ShapeDtypeStruct((NYC, NB // 2, LANES), F32),
        ],
        scratch_shapes=[pltpu.VMEM((NZ * GROWS, NC * LANES), BF16)],
        compiler_params=params(),
        name="gram",
    )(placed, *parts)


def matmul(left, right):
    return jnp.dot(left, right, preferred_element_type=F32, precision=lax.Precision.HIGHEST)


def whiten_kernel(points, in_ref, out_ref):
    total = jnp.sum(in_ref[...], axis=0)
    rows = lax.broadcasted_iota(jnp.int32, (NB, NB), 0)
    cols = lax.broadcasted_iota(jnp.int32, (NB, NB), 1)
    two_rows = lax.broadcasted_iota(jnp.int32, (2 * NB, 2 * NB), 0)
    two_cols = lax.broadcasted_iota(jnp.int32, (2 * NB, 2 * NB), 1)
    identity = (two_rows == two_cols).astype(F32)
    flip = (two_rows < NB) == (two_cols >= NB)
    sign = jnp.where(flip, -1.0, 1.0)
    iterates, inverses, scales, energies = [], [], [], []
    for i in range(2):
        pair = total[:, i * 2 * NB : (i + 1) * 2 * NB]
        packed = jnp.concatenate([pair[:, :NB], pair[:, NB:]], axis=0)
        lower = jnp.where(rows > cols, packed, 0.0)
        diagonal = jnp.where(rows == cols, packed, 0.0)
        upper = jnp.where(rows < cols, packed, 0.0)
        real = lower + lower.T + diagonal
        imag = upper - upper.T
        hermit = jnp.concatenate(
            [
                jnp.concatenate([real, -imag], axis=1),
                jnp.concatenate([imag, real], axis=1),
            ],
            axis=0,
        )
        frob = jnp.sqrt(jnp.sum(hermit * hermit, keepdims=True) + 1e-06)
        iterates.append(hermit / frob)
        inverses.append(identity)
        scales.append(jnp.sqrt(6.0 * points / frob))
        energies.append(jnp.sum(diagonal, keepdims=True) / (3.0 * NB * points))
    for _ in range(NSIT):
        for i in range(2):
            factor = 1.5 * identity - 0.5 * matmul(inverses[i], iterates[i])
            iterates[i] = matmul(iterates[i], factor)
            inverses[i] = matmul(factor, inverses[i])
    out_ref[: 2 * NB, :] = jnp.concatenate(
        [inverses[i] * sign * scales[i] for i in range(2)], axis=1
    ).astype(BF16)
    energy = jnp.concatenate(
        [jnp.broadcast_to(energies[i], (1, 2 * NB)) for i in range(2)], axis=1
    )
    high = energy.astype(BF16)
    middle = (energy - high.astype(F32)).astype(BF16)
    low = (energy - high.astype(F32) - middle.astype(F32)).astype(BF16)
    zero = jnp.zeros((5, LANES), BF16)
    out_ref[2 * NB :, :] = jnp.concatenate([high, middle, low, zero], axis=0)


def whiten(grams, points):
    return pl.pallas_call(
        functools.partial(whiten_kernel, points),
        in_specs=[VMEM],
        out_specs=VMEM,
        out_shape=jax.ShapeDtypeStruct((2 * NB + 8, LANES), BF16),
        compiler_params=params(),
        name="whiten",
    )(grams)


def modes_kernel(coef_ref, spec_ref, modes_ref, energy_ref):
    n = NC * 2 * NB
    rows = lax.broadcasted_iota(jnp.int32, (n, 2 * NB), 0)
    cols = lax.broadcasted_iota(jnp.int32, (n, 2 * NB), 1)
    source = (rows % 2) * NB + rows // (2 * NC)
    pick = (source == cols).astype(BF16)
    wide_rows = lax.broadcasted_iota(jnp.int32, (n, n), 0)
    wide_cols = lax.broadcasted_iota(jnp.int32, (n, n), 1)
    keep = (wide_rows // 2) % NC == wide_cols // (2 * NB)
    lane = lax.broadcasted_iota(jnp.int32, (8, LANES), 1)
    energy = jnp.zeros((8, LANES), F32)
    for d in range(NYC):
        for i in range(2):
            f = 2 * d + i
            part = jnp.dot(
                pick,
                coef_ref[d, : 2 * NB, i * 2 * NB : (i + 1) * 2 * NB],
                preferred_element_type=F32,
            )
            wide = jnp.where(keep, jnp.concatenate([part] * NC, axis=1), 0.0).astype(BF16)
            modes_ref[f * n : (f + 1) * n, :] = jnp.dot(
                wide, spec_ref[f], preferred_element_type=F32
            ).astype(BF16)
            tail = coef_ref[d, 2 * NB :, :].astype(F32)
            value = tail[0:1] + tail[1:2] + tail[2:3]
            value = value[:, i * 2 * NB : i * 2 * NB + 1]
            energy = jnp.where(lane == f, value, energy)
    energy_ref[...] = energy


def modes(coefs, spec):
    return pl.pallas_call(
        modes_kernel,
        in_specs=[VMEM, VMEM],
        out_specs=[VMEM, VMEM],
        out_shape=[
            jax.ShapeDtypeStruct((NF * NB * NC * 2, LANES), BF16),
            jax.ShapeDtypeStruct((8, LANES), F32),
        ],
        compiler_params=params(),
        name="modes",
    )(coefs, spec)


def local(snapshots, block_starts, freq_index):
    x = jnp.transpose(snapshots, (1, 0, 2))
    packs = [pack(x, comps) for comps in CHUNKS]
    w, placed = tables(block_starts, dft_rows(freq_index))

    arrived = [send_yc(a, k) for k, a in enumerate(packs[0])]
    spectra = []
    for q in range(len(CHUNKS)):
        parts = dft(w, arrived)
        if q + 1 < len(CHUNKS):
            parts, following = lax.optimization_barrier((parts, packs[q + 1]))
            arrived, out = [], []
            for k in range(NYC):
                arrived.append(send_yc(following[k], k))
                out.append(send_z(parts[k], k))
        else:
            out = [send_z(a, k) for k, a in enumerate(parts)]
        spectra += out
    spec, grams = gram(placed, spectra)

    grams = lax.all_to_all(grams, ("y", "c"), split_axis=0, concat_axis=0, tiled=True).sum(axis=0)
    grams = jnp.broadcast_to(grams, (NZ * NX, *grams.shape))
    grams = lax.all_to_all(grams, ("z", "x"), split_axis=0, concat_axis=0, tiled=True)
    points = float(LANES * NZ * NY * NCORE * NX)
    coefs = whiten(grams, points)
    coefs = jnp.broadcast_to(coefs, (NYC, *coefs.shape))
    coefs = lax.all_to_all(coefs, ("y", "c"), split_axis=0, concat_axis=0, tiled=True)
    out, energy = modes(coefs, spec)
    out = jnp.transpose(out.reshape(NF, NB, NC, 2, LANES), (0, 1, 3, 2, 4))
    return out, energy[0, :NF]


def solution(mesh):
    split = Mesh(mesh.devices.reshape(NZ, NY, NCORE, NX), ("z", "y", "c", "x"))
    return jax.shard_map(
        local,
        mesh=split,
        in_specs=(P(("z", "y", "c"), None, "x"), P(), P()),
        out_specs=(P(None, None, None, None, ("x", "z", "y", "c")), P()),
        check_vma=False,
    )
```
